32 devices in a mesh: grp: 8 (over z, core), blk: 4 (over y, x).
Axes of the slice: x: 2, y: 2, z: 4, core: 2. Of those that a mesh axis runs over, the one named last changes fastest.
Arguments:
- patches: float32 [256, 32, 1024], P(('grp', 'blk')), may hold values from -6 to 6
- counts: int32 [32], P(('grp', 'blk')), may hold values from 1 to 8
- moves: int32 [32, 4], P(('grp', 'blk')), may hold values from 0 to 3, as said below
- tags: int32 [8, 32], P('grp'), may hold values from 0 to 3
Outputs:
- fine: bfloat16 [256, 64, 4096], P(('grp', 'blk'))
The draws below stay inside these ranges and needn't reach their ends.
Inputs may be any that keep to these rules, and one draw needn't show every extreme that they name: `moves`: each device holds between 1 and 8 live patches before and after every diffusion step, and hands on fewer patches than it holds at that step; in every draw some device hands on exactly 3 patches in some step.
All inputs are finite; a program needn't handle non-finite values.
Results may differ from the reference program's by a relative error of at most 0.001.
Values sent between devices are 32-bit elements; how exact they have to be, the bound alone decides.
No kernel may reach another device: no remote copies, remote signals or barrier semaphores. Data moves between devices by JAX's collectives and lax.ppermute only.
A program may use at most 128 MiB of HBM per device.

```python
import jax
import jax.numpy as jnp
from jax import lax

E = 32
CAP = 8
MOST = 3
STEPS = 4
NDEV = 32
NBOX = 32
NPATCH = 256
N_GRP = 8
N_BLK = 4


def plan_loads(key):
    key = jax.random.fold_in(key, 7)
    first, second, third, fourth = jax.random.split(key, 4)
    groups = NDEV // N_BLK
    heavy = jax.random.randint(first, (groups, N_BLK), 0, 2) == 0
    large = jax.random.randint(second, (groups, N_BLK), CAP // 2, CAP + 1)
    small = jax.random.randint(third, (groups, N_BLK), 2, min(5, CAP + 1))
    live = jnp.where(heavy, large, small)
    live = live.at[:, 0].set(jnp.maximum(live[:, 0], MOST + 1))
    live = live.at[:, 1].set(jnp.minimum(live[:, 1], CAP - MOST))
    wishes = jax.random.randint(fourth, (groups, N_BLK, STEPS), 0, MOST + 1)
    wishes = wishes.at[:, 0, 0].set(MOST)
    initial = live
    columns = []
    for step in range(STEPS):
        following = jnp.roll(live, -1, axis=1)
        handed = jnp.minimum(jnp.minimum(wishes[:, :, step], live - 1), CAP - following)
        columns.append(handed)
        live = live - handed + jnp.roll(handed, 1, axis=1)
    return (initial.reshape(NDEV).astype(jnp.int32), jnp.stack(columns, -1).reshape(NDEV, STEPS).astype(jnp.int32))


def draw_counts(key, part):
    return plan_loads(key)[0]


def draw_moves(key, part):
    return plan_loads(key)[1]


def touch_ends(values, key, smallest, top_value):
    longest = values.shape.index(max(values.shape))
    spots = []
    for shift in (0, 1):
        where = [jax.random.randint(jax.random.fold_in(key, axis), (), 0, length) for axis, length in enumerate(values.shape)]
        where[longest] = (where[longest] + shift) % values.shape[longest]
        spots.append(tuple(where))
    return values.at[spots[0]].set(smallest).at[spots[1]].set(top_value)


def block_scale(rng, extent, cuts, least, high):
    factor_of = 1.0
    for dim, shards_of in cuts:
        draws = jax.random.uniform(jax.random.fold_in(jax.random.fold_in(rng, 6), dim), (shards_of,), jnp.float32, least / len(cuts), high / len(cuts))
        factor_of = factor_of * jnp.repeat(jnp.exp(draws), extent[dim] // shards_of).reshape((-1,) + (1,) * (len(extent) - 1 - dim))
    return factor_of


def gaussian(key, shape, scale, reach, cuts=(), kind=jnp.bfloat16):
    drawn = jax.random.normal(key, shape, jnp.float32) * scale
    if len(cuts) > 0:
        drawn = block_scale(key, shape, cuts, -0.22, 0.18) * drawn
    return jnp.clip(drawn, min=-reach, max=reach).astype(kind)


def setup_inputs(seed: int = 0) -> dict:
    keys = jax.random.split(jax.random.key(seed), 5)
    patches = gaussian(keys[0], (NPATCH, E, E * E), 1.0, 6.0, ((0, 32),), jnp.float32)
    counts = draw_counts(jax.random.fold_in(keys[4], 71), 0)
    moves = draw_moves(jax.random.fold_in(keys[4], 71), 0)
    tags = touch_ends(jax.random.randint(keys[3], (N_GRP, NBOX), 0, 4), jax.random.fold_in(keys[3], 1), 0, 3).astype(jnp.int32)
    return dict(patches=patches, counts=counts, moves=moves, tags=tags)


def refine_table(edge, margin):
    finer = jnp.arange(2 * edge)[:, None]
    coarse = jnp.arange(edge + 2 * margin)[None, :]
    home = finer // 2 + margin
    side = home + 2 * (finer % 2) - 1
    return (0.75 * (coarse == home) + 0.25 * (coarse == side)).astype(jnp.float32)


def refine(extended, edge):
    number = extended.shape[0]
    cube = extended.reshape(number, edge + 2, edge, edge)
    across = refine_table(edge, 1)
    inner = refine_table(edge, 0)
    highest = lax.Precision.HIGHEST
    first = jnp.einsum('fx,pxyz->pfyz', across, cube, precision=highest)
    second = jnp.einsum('gy,pfyz->pfgz', inner, first, precision=highest)
    third = jnp.einsum('hz,pfgz->pfgh', inner, second, precision=highest)
    return third.reshape(number, 2 * edge, 4 * edge * edge)


def tag_factors(tag_row, offset, capacity):
    position = offset + jnp.arange(capacity).astype(jnp.int32)
    boxes = jnp.arange(tag_row.shape[0]).astype(jnp.int32)
    picked = jnp.sum(jnp.where(position[:, None] == boxes[None, :], tag_row[None, :], 0), axis=1)
    return 1.0 + 0.5 * picked.astype(jnp.float32)


def finish(work, live, lower, upper, factors):
    capacity, edge = work.shape[0], work.shape[1]
    slots = jnp.arange(capacity).astype(jnp.int32)
    below = jnp.concatenate([lower[None], work[:-1, edge - 1]], 0)
    above = jnp.concatenate([work[1:, 0], upper[None]], 0)
    above = jnp.where((slots == live - 1)[:, None], upper[None], above)
    extended = jnp.concatenate([below[:, None], work, above[:, None]], 1)
    refined = refine(extended, edge)
    scaled = refined * factors[:, None, None]
    return jnp.where((slots < live)[:, None, None], scaled, 0.0).astype(jnp.bfloat16)


def reference(patches, counts, moves, tags):
    groups = N_GRP
    cycle = N_BLK
    field = patches.reshape(groups, cycle, CAP, E, E * E)
    field = jnp.concatenate([field, jnp.zeros((groups, cycle, MOST, E, E * E), field.dtype)], 2)
    live = counts.reshape(groups, cycle)
    handed = moves.reshape(groups, cycle, STEPS)
    cutter = jax.vmap(jax.vmap(lambda block, first: lax.dynamic_slice_in_dim(block, first, MOST, 0)))
    paster = jax.vmap(jax.vmap(lambda block, piece, first: lax.dynamic_update_slice_in_dim(block, piece, first, 0)))
    for step in range(STEPS):
        sent = handed[:, :, step]
        start = live - sent
        parcel = cutter(field, start)
        arrived = jnp.roll(parcel, 1, axis=1)
        field = paster(field, arrived, start)
        live = start + jnp.roll(sent, 1, axis=1)
    offsets = (jnp.cumsum(live, axis=1) - live).reshape(NDEV)
    work = field[:, :, :CAP].reshape(NDEV, CAP, E, E * E)
    live = live.reshape(NDEV)
    tops = work[jnp.arange(NDEV), live - 1, E - 1]
    zero_plane = jnp.zeros((1, E * E), work.dtype)
    lower = jnp.concatenate([zero_plane, tops[:-1]], 0)
    upper = jnp.concatenate([work[1:, 0, 0], zero_plane], 0)
    group_tags = jnp.repeat(tags, cycle, axis=0)

    def one_device(items):
        block, count, below, above, offset, tag_row = items
        return finish(block, count, below, above, tag_factors(tag_row, offset, CAP))

    result = lax.map(one_device, (work, live, lower, upper, offsets, group_tags))
    return result.reshape(NDEV * CAP, 2 * E, 4 * E * E)
```

```python
import functools

import jax
import jax.numpy as jnp
import numpy as np
from jax import lax
from jax.experimental import pallas as pl
from jax.experimental.pallas import tpu as pltpu
from jax.sharding import PartitionSpec as P

MOST = 3
STEPS = 4
LANES = 128


def passed_along(block, axis, distance):
    devices = range(lax.axis_size(axis))
    route = [((i - distance) % len(devices), i) for i in devices]
    return lax.ppermute(block, axis, route)


def entering(value, axis, join, neutral):
    count, mine = (lax.axis_size(axis), lax.axis_index(axis))
    pieces = lax.all_gather(value, axis)
    running = jnp.full_like(value, 0) + jnp.asarray(neutral, value.dtype)

    def hop(position, running):
        longer = join(running, pieces[position])
        return jnp.where(position < mine, longer, running)

    return lax.fori_loop(0, count - 1, hop, running)


def from_behind(x, axis, by):
    devices = lax.axis_size(axis)
    pairs = [(i, i + by) for i in range(devices) if 0 <= i + by < devices]
    return lax.ppermute(x, axis, pairs)


def refine_table(edge, ghosts):
    finer = np.arange(2 * edge)[:, None]
    coarse = np.arange(edge + 2 * ghosts)[None, :]
    home = finer // 2 + ghosts
    side = home + 2 * (finer % 2) - 1
    return 0.75 * (coarse == home) + 0.25 * (coarse == side)


def window_table(edge):
    inner = LANES // edge - 2
    along_y = refine_table(inner, 1)
    along_z = refine_table(edge, 0)
    table = np.kron(along_y, along_z).T
    return jnp.asarray(np.concatenate([table, table], 0), jnp.bfloat16)


def refine_kernel(live_ref, factor_ref, work_ref, lower_ref, upper_ref, table_ref, out_ref, rows_ref, split_ref):
    capacity, edge, plane = work_ref.shape
    slot = pl.program_id(0)
    live = live_ref[0]

    @pl.when(slot >= live)
    def _():
        out_ref[...] = jnp.zeros_like(out_ref)

    @pl.when(slot < live)
    def _():
        factor = factor_ref[slot]
        middle = work_ref[slot]
        before = work_ref[jnp.maximum(slot - 1, 0), edge - 1 : edge, :]
        after = work_ref[jnp.minimum(slot + 1, capacity - 1), 0:1, :]
        before = jnp.where(slot == 0, lower_ref[...], before)
        after = jnp.where(slot == live - 1, upper_ref[...], after)
        place = lax.broadcasted_iota(jnp.int32, middle.shape, 0)
        below = jnp.where(place == 0, before, pltpu.roll(middle, 1, 0))
        above = jnp.where(place == edge - 1, after, pltpu.roll(middle, edge - 1, 0))
        home = middle * (0.75 * factor)
        even = home + below * (0.25 * factor)
        odd = home + above * (0.25 * factor)
        for u in range(plane // LANES):
            cut = slice(u * LANES, (u + 1) * LANES)
            rows_ref[u, pl.ds(0, edge, 2), :] = even[:, cut]
            rows_ref[u, pl.ds(1, edge, 2), :] = odd[:, cut]
        rows = jnp.concatenate([rows_ref[u] for u in range(plane // LANES)], axis=1)
        lane = lax.broadcasted_iota(jnp.int32, rows.shape, 1)
        later = jnp.where(lane < edge, 0.0, pltpu.roll(rows, edge, 1))
        sooner = jnp.where(lane >= plane - edge, 0.0, pltpu.roll(rows, plane - edge, 1))
        for side, moved in enumerate((later, sooner)):
            high = moved.astype(jnp.bfloat16)
            low = (moved - high.astype(jnp.float32)).astype(jnp.bfloat16)
            for u in range(plane // LANES):
                cut = slice(u * LANES, (u + 1) * LANES)
                split_ref[2 * u + side, :, :LANES] = high[:, cut]
                split_ref[2 * u + side, :, LANES:] = low[:, cut]
        windows, fine, depth = split_ref.shape
        width = table_ref.shape[1]
        table = table_ref[...]
        group = 4
        for g in range(0, windows, group):
            left = split_ref[g : g + group].reshape(group * fine, depth)
            product = jnp.dot(left, table, preferred_element_type=jnp.float32)
            for i in range(group):
                out_ref[0, :, (g + i) * width : (g + i + 1) * width] = product[i * fine : (i + 1) * fine].astype(jnp.bfloat16)


def refine(work, live, lower, upper, factors):
    capacity, edge, plane = work.shape
    table = window_table(edge)
    windows = 2 * plane // LANES
    whole = lambda *shape: pl.BlockSpec(shape, lambda i, *_: (0,) * len(shape))
    return pl.pallas_call(
        refine_kernel,
        out_shape=jax.ShapeDtypeStruct((capacity, 2 * edge, 4 * plane), jnp.bfloat16),
        grid_spec=pltpu.PrefetchScalarGridSpec(
            num_scalar_prefetch=2,
            grid=(capacity,),
            in_specs=[whole(capacity, edge, plane), whole(1, plane), whole(1, plane), whole(*table.shape)],
            out_specs=pl.BlockSpec((1, 2 * edge, 4 * plane), lambda i, *_: (i, 0, 0)),
            scratch_shapes=[
                pltpu.VMEM((plane // LANES, 2 * edge, LANES), jnp.float32),
                pltpu.VMEM((windows, 2 * edge, 2 * LANES), jnp.bfloat16),
            ],
        ),
        name="refine",
    )(live.reshape(1), factors, work, lower[None], upper[None], table)


def tag_factors(tag_row, offset, capacity):
    position = offset + jnp.arange(capacity)
    boxes = jnp.arange(tag_row.shape[0])
    picked = jnp.sum(jnp.where(position[:, None] == boxes[None, :], tag_row[None, :], 0), axis=1)
    return 1.0 + 0.5 * picked.astype(jnp.float32)


def add_counts(earlier, later):
    return earlier + later


def body(patches, counts, moves, tags):
    capacity, edge = (patches.shape[0], patches.shape[1])
    live = counts[0]
    padding = jnp.zeros((MOST,) + patches.shape[1:], patches.dtype)
    field = jnp.concatenate([patches, padding], 0)
    earlier = passed_along(moves, "blk", 1)
    for step in range(STEPS):
        start = live - moves[0, step]
        parcel = lax.dynamic_slice_in_dim(field, start, MOST, 0)
        arrived = passed_along(parcel, "blk", 1)
        field = lax.dynamic_update_slice_in_dim(field, arrived, start, 0)
        live = start + earlier[0, step]
    work = field[:capacity]
    offset = entering(live.reshape(1), "blk", add_counts, jnp.zeros((1,), jnp.int32))[0]
    top_patch = lax.dynamic_index_in_dim(work, live - 1, 0, keepdims=False)
    lower = from_behind(top_patch[edge - 1], ("grp", "blk"), 1)
    upper = from_behind(work[0, 0], ("grp", "blk"), -1)
    return refine(work, live, lower, upper, tag_factors(tags[0], offset, capacity))


def solution(mesh):
    in_specs = (
        P(("grp", "blk"), None, None),
        P(("grp", "blk")),
        P(("grp", "blk"), None),
        P("grp", None),
    )
    out_specs = P(("grp", "blk"), None, None)
    return jax.shard_map(body, mesh=mesh, in_specs=in_specs, out_specs=out_specs, check_vma=False)
```

```python
import functools
import itertools

import jax
import jax.numpy as jnp
import numpy as np
from jax import lax
from jax.experimental import pallas as pl
from jax.experimental.pallas import tpu as pltpu
from jax.sharding import PartitionSpec as P


LANES = 128
SUBLANES = 8
CHOICES = (
    (4, 3, 3), (5, 4, 4), (3, 2, 2), (2, 4, 2), (2, 2, 2), (3, 5, 3), (3, 3, 3), (5, 2, 2), (4, 2, 2),
    (2, 3, 2), (2, 2, 3), (4, 1, 1), (1, 3, 1), (1, 1, 2), (3, 1, 1), (5, 1, 1), (1, 2, 1), (2, 2, 4),
    (6, 1, 1), (2, 1, 1), (2, 5, 2), (1, 1, 3), (1, 4, 1), (3, 4, 1), (3, 3, 1), (5, 3, 3), (1, 1, 1),
    (3, 2, 1), (1, 5, 1), (2, 2, 1), (2, 3, 1), (3, 1, 2), (4, 3, 1), (2, 1, 2), (4, 2, 1), (1, 2, 2),
)


def refine_table(edge, ghosts):
    finer = np.arange(2 * edge)[:, None]
    coarse = np.arange(edge + 2 * ghosts)[None, :]
    home = finer // 2 + ghosts
    side = home + 2 * (finer % 2) - 1
    return 0.75 * (coarse == home) + 0.25 * (coarse == side)


def window_table(edge):
    inner = LANES // edge - 2
    along_y = refine_table(inner, 1)
    along_z = refine_table(edge, 0)
    table = np.kron(along_y, along_z).T
    return jnp.asarray(np.concatenate([table, table], 0), jnp.bfloat16)


def refine_kernel(plan_ref, tag_ref, held_ref, work_ref, ends_ref, before_ref, table_ref, out_ref, rows_ref, split_ref):
    capacity = work_ref.shape[0]
    fine = out_ref.shape[1]
    edge, plane = (fine // 2, out_ref.shape[2] // 4)
    across = plane // LANES
    slot = pl.program_id(0)
    live = plan_ref[2, 0]

    @pl.when(slot >= live)
    def _():
        out_ref[...] = jnp.zeros_like(out_ref)

    @pl.when(slot < live)
    def _():
        factor = 1.0 + 0.5 * tag_ref[0, plan_ref[2, 1] + slot].astype(jnp.float32)

        def part(j, tiles, rows):
            j = jnp.clip(j, 0, capacity - 1)
            return jnp.where(plan_ref[0, j] == 0, held_ref[j, tiles, rows], work_ref[j, tiles, rows])

        def flat(tiles):
            tiles = tiles.reshape(-1, across, tiles.shape[-2], LANES)
            return jnp.concatenate([tiles[:, u].reshape(-1, LANES) for u in range(across)], axis=1)

        middle = flat(part(slot, slice(None), slice(None)))
        before = part(slot - 1, slice(edge // SUBLANES * across - across, None), slice(SUBLANES - 1, None))
        after = part(slot + 1, slice(0, across), slice(0, 1))
        lower = jnp.where(plan_ref[2, 4] == 0, ends_ref[0], before_ref[...])
        before = jnp.where(slot == 0, lower[:, None, :], before)
        after = jnp.where(slot == live - 1, ends_ref[1][:, None, :], after)
        before, after = flat(before), flat(after)
        place = lax.broadcasted_iota(jnp.int32, middle.shape, 0)
        below = jnp.where(place == 0, before, pltpu.roll(middle, 1, 0))
        above = jnp.where(place == edge - 1, after, pltpu.roll(middle, edge - 1, 0))
        home = middle * (0.75 * factor)
        even = home + below * (0.25 * factor)
        odd = home + above * (0.25 * factor)
        for u in range(plane // LANES):
            cut = slice(u * LANES, (u + 1) * LANES)
            rows_ref[u, pl.ds(0, edge, 2), :] = even[:, cut]
            rows_ref[u, pl.ds(1, edge, 2), :] = odd[:, cut]
        rows = jnp.concatenate([rows_ref[u] for u in range(plane // LANES)], axis=1)
        lane = lax.broadcasted_iota(jnp.int32, rows.shape, 1)
        later = jnp.where(lane < edge, 0.0, pltpu.roll(rows, edge, 1))
        sooner = jnp.where(lane >= plane - edge, 0.0, pltpu.roll(rows, plane - edge, 1))
        for side, moved in enumerate((later, sooner)):
            high = moved.astype(jnp.bfloat16)
            low = (moved - high.astype(jnp.float32)).astype(jnp.bfloat16)
            for u in range(plane // LANES):
                cut = slice(u * LANES, (u + 1) * LANES)
                split_ref[2 * u + side, :, :LANES] = high[:, cut]
                split_ref[2 * u + side, :, LANES:] = low[:, cut]
        windows, fine, depth = split_ref.shape
        width = table_ref.shape[1]
        table = table_ref[...]
        group = 4
        for g in range(0, windows, group):
            left = split_ref[g : g + group].reshape(group * fine, depth)
            product = jnp.dot(left, table, preferred_element_type=jnp.float32)
            for i in range(group):
                out_ref[0, :, (g + i) * width : (g + i + 1) * width] = product[i * fine : (i + 1) * fine].astype(jnp.bfloat16)


def refine(held, work, plan, tags, ends, before, edge):
    capacity, parts = work.shape[:2]
    plane = parts * SUBLANES * LANES // edge
    table = window_table(edge)
    windows = 2 * plane // LANES
    whole = lambda x: pl.BlockSpec(x.shape, lambda i, *_: (0,) * x.ndim)
    operands = (held, work, ends, before, table)
    return pl.pallas_call(
        refine_kernel,
        out_shape=jax.ShapeDtypeStruct((capacity, 2 * edge, 4 * plane), jnp.bfloat16),
        grid_spec=pltpu.PrefetchScalarGridSpec(
            num_scalar_prefetch=2,
            grid=(capacity,),
            in_specs=[whole(x) for x in operands],
            out_specs=pl.BlockSpec((1, 2 * edge, 4 * plane), lambda i, *_: (i, 0, 0)),
            scratch_shapes=[
                pltpu.VMEM((plane // LANES, 2 * edge, LANES), jnp.float32),
                pltpu.VMEM((windows, 2 * edge, 2 * LANES), jnp.bfloat16),
            ],
        ),
        compiler_params=pltpu.CompilerParams(vmem_limit_bytes=16 << 20),
        name="refine",
    )(plan, tags, *operands)


def swap(block, axis, bit):
    return lax.ppermute(block, axis, [(i, i ^ bit) for i in range(lax.axis_size(axis))])


def all_of(rows, axis):
    count, bit = (lax.axis_size(axis), 1)
    while bit < count:
        other = swap(rows, axis, bit)
        rows = jnp.concatenate([rows, other], 0)
        bit *= 2
    return rows


def forward(block, axis, distance):
    count = lax.axis_size(axis)
    return lax.ppermute(block, axis, [(i, (i + distance) % count) for i in range(count)])


def capacity_choices(distances, capacity):
    most = capacity - 1
    if distances == 3:
        choices = set(CHOICES)
    else:
        choices = {(u,) * distances for u in (1, 2, 3, 4)}
    choices = {tuple(min(c, most) for c in choice) for choice in choices} | {(most,) * distances}
    load = lambda c: (max(a + b for a, b in itertools.combinations(c + (0, 0), 2)), sum(c), c)
    return sorted(choices, key=load)


def tiled(patches):
    capacity, edge, plane = patches.shape
    cut = patches.reshape(capacity, edge // SUBLANES, SUBLANES, plane // LANES, LANES)
    return cut.transpose(0, 1, 3, 2, 4).reshape(capacity, -1, SUBLANES, LANES)


def last_plane(patches_ref, slot):
    return patches_ref.at[slot, pl.ds(patches_ref.shape[1] - SUBLANES, SUBLANES), SUBLANES - 1]


def first_plane(patches_ref, slot):
    return patches_ref.at[slot, pl.ds(0, SUBLANES), 0]


def plan_kernel(given_ref, plan_ref, pick_ref, *, choices, capacity, steps):
    devices = given_ref.shape[0]
    count = devices * max(1, SUBLANES // devices)
    shape = (count, LANES)
    wide = lambda column: jnp.broadcast_to(column, shape)
    behind = lambda x, k: pltpu.roll(x, k % count, 0) if k % count else x
    lane = lax.broadcasted_iota(jnp.int32, shape, 1)
    row = lax.broadcasted_iota(jnp.int32, shape, 0)
    given = given_ref[...]
    mine = given[0:1, steps + 1 : steps + 2]
    rows = jnp.zeros(shape, jnp.int32)
    for f in range(devices):
        ahead = given[f : f + 1, steps + 1 : steps + 2] - mine
        here = row % devices == jnp.where(ahead < 0, ahead + devices, ahead)
        rows = jnp.where(here, wide(given[f : f + 1]), rows)

    def trace(rows):
        starts, live = [], wide(rows[:, 0:1])
        for step in range(steps):
            sent = wide(rows[:, step + 1 : step + 2])
            starts.append(live - sent)
            live = starts[-1] + behind(sent, 1)
        back, place = jnp.zeros(shape, jnp.int32), lane
        for step in reversed(range(steps)):
            here, there = starts[step], behind(starts[step], 1)
            for k in range(1, steps - step):
                here = jnp.where(back == k, behind(starts[step], k), here)
                there = jnp.where(back == k, behind(starts[step], k + 1), there)
            came = place >= here
            place = jnp.where(came, place - here + there, place)
            back = jnp.where(came, back + 1, back)
        for _ in range(steps // devices):
            back = jnp.where(back >= devices, back - devices, back)
        return live, back, place

    def at_top(live, values):
        picked = jnp.where(lane == live - 1, values, 0).astype(jnp.float32)
        return wide(jnp.sum(picked, axis=1, keepdims=True)).astype(jnp.int32)

    live, back, place = trace(rows)
    start_flag = (wide(mine) == 0).astype(jnp.int32)
    top_back = behind(at_top(live, back), 1)
    top_place = jnp.clip(behind(at_top(live, place), 1), 0, capacity - 1)
    top_from = jnp.where(top_back + 1 >= devices, 0, top_back + 1)

    filled = lane < live
    source = jnp.where(filled, back, -1)
    rank = jnp.zeros(shape, jnp.int32)
    for j in range(capacity):
        rank = jnp.where((wide(source[:, j : j + 1]) == source) & (lane > j), rank + 1, rank)
    code = jnp.where(source == row, rank, -1)
    sent = jnp.zeros(shape, jnp.int32)
    for j in range(capacity):
        sent = jnp.where(wide(code[:, j : j + 1]) == lane, wide(place[:, j : j + 1]), sent)
    fits = None
    for k in range(len(choices[0])):
        limit = jnp.full((1, LANES), -1.0, jnp.float32)
        for i, choice in enumerate(choices):
            limit = jnp.where(lane[:1] == i, float(choice[k]), limit)
        hits = jnp.sum((source == k + 1).astype(jnp.float32), axis=1, keepdims=True)
        fit = jnp.max(hits, axis=0, keepdims=True) <= limit
        fits = fit if fits is None else fits & fit
    pick = jnp.min(jnp.where(fits, lane[:1].astype(jnp.float32), LANES - 1.0), axis=1, keepdims=True).astype(jnp.int32)
    pick_ref[...] = jnp.broadcast_to(pick, pick_ref.shape)
    lower = (wide(rows[:, steps + 1 : steps + 2]) < wide(mine)) & (row < devices)
    offset = jnp.sum(jnp.where(lower, live, 0).astype(jnp.float32), axis=0, keepdims=True).astype(jnp.int32)
    kind = jnp.maximum(source, 0)
    index = jnp.where(kind > 0, rank, jnp.where(filled, place, 0))
    values = [wide(live[:1]), wide(offset), wide(top_from[:1]), wide(top_place[:1]), start_flag]
    sizes = values[0]
    for i, value in enumerate(values[1:], 1):
        sizes = jnp.where(lane == i, value, sizes)
    sent = jnp.where(lane == capacity, top_place, sent)
    table = jnp.where(row == 0, wide(kind[:1]), jnp.where(row == 1, wide(index[:1]), sizes))
    plan_ref[...] = jnp.where(row > 2, behind(sent, 2), table)


def make_plan(given, choices, capacity, steps):
    devices = given.shape[0]
    count = devices * max(1, SUBLANES // devices)
    return pl.pallas_call(
        functools.partial(plan_kernel, choices=choices, capacity=capacity, steps=steps),
        out_shape=[jax.ShapeDtypeStruct((rows, LANES), jnp.int32) for rows in (count, 1)],
        in_specs=[pl.BlockSpec(memory_space=pltpu.VMEM)],
        out_specs=[pl.BlockSpec(memory_space=pltpu.VMEM)] * 2,
        compiler_params=pltpu.CompilerParams(vmem_limit_bytes=1 << 20),
        name="plan",
    )(given)


def pack_kernel(sizes, last, plan_ref, patches_ref, after_ref, *refs):
    parcels, sems = refs[:-1], refs[-1]
    capacity, parts = patches_ref.shape[:2]

    def each(act):
        used = 0
        for k, (size, parcel) in enumerate(zip(sizes, parcels)):

            @pl.loop(0, size)
            def _(r, k=k, parcel=parcel, used=used):
                act(pltpu.make_async_copy(patches_ref.at[plan_ref[3 + k, r]], parcel.at[pl.ds(r * parts, parts)], sems.at[used + r]))

            used += size
            act(pltpu.make_async_copy(last_plane(patches_ref, plan_ref[3 + k, capacity]), parcel.at[size * parts], sems.at[used]))
            used += 1
            if k == last:
                upper = parcel.at[size * parts + 1]

                @pl.when(plan_ref[2, 4] == 0)
                def _():
                    act(pltpu.make_async_copy(first_plane(patches_ref, 0), upper, sems.at[used]))

                @pl.when(plan_ref[2, 4] != 0)
                def _():
                    act(pltpu.make_async_copy(after_ref, upper, sems.at[used]))

                used += 1

    each(lambda copy: copy.start())
    each(lambda copy: copy.wait())


def pack(plan, patches, after, sizes, last):
    parts = patches.shape[1]
    return pl.pallas_call(
        functools.partial(pack_kernel, sizes, last),
        out_shape=[
            jax.ShapeDtypeStruct((size * parts + 1 + (k == last),) + patches.shape[2:], patches.dtype)
            for k, size in enumerate(sizes)
        ],
        grid_spec=pltpu.PrefetchScalarGridSpec(
            num_scalar_prefetch=1,
            grid=(),
            in_specs=[pl.BlockSpec(memory_space=pl.ANY)] * 2,
            out_specs=[pl.BlockSpec(memory_space=pl.ANY) for _ in sizes],
            scratch_shapes=[pltpu.SemaphoreType.DMA((sum(sizes) + len(sizes) + 1,))],
        ),
        compiler_params=pltpu.CompilerParams(vmem_limit_bytes=1 << 20),
        name="pack",
    )(plan, patches, after)


def settle_kernel(plan_ref, patches_ref, held_ref, sems):
    def each(act):
        @pl.loop(0, held_ref.shape[0])
        def _(j):
            act(pltpu.make_async_copy(patches_ref.at[plan_ref[1, j]], held_ref.at[j], sems.at[j]))

    each(lambda copy: copy.start())
    each(lambda copy: copy.wait())


def settle(plan, patches):
    return pl.pallas_call(
        settle_kernel,
        out_shape=jax.ShapeDtypeStruct(patches.shape, patches.dtype),
        grid_spec=pltpu.PrefetchScalarGridSpec(
            num_scalar_prefetch=1,
            grid=(),
            in_specs=[pl.BlockSpec(memory_space=pl.ANY)],
            out_specs=pl.BlockSpec(memory_space=pl.ANY),
            scratch_shapes=[pltpu.SemaphoreType.DMA((patches.shape[0],))],
        ),
        compiler_params=pltpu.CompilerParams(vmem_limit_bytes=1 << 20),
        cost_estimate=pl.CostEstimate(flops=1 << 24, bytes_accessed=1 << 21, transcendentals=0),
        name="settle",
    )(plan, patches)


def assemble_kernel(sizes, last, plan_ref, patches_ref, after_ref, *refs):
    parcels, work_ref, ends_ref, sems = refs[:-3], refs[-3], refs[-2], refs[-1]
    capacity, parts = work_ref.shape[:2]

    def put(source, side):
        pltpu.make_async_copy(source, ends_ref.at[side], sems.at[capacity + side]).start()

    origin, slot = plan_ref[2, 2], plan_ref[2, 3]
    for k, (size, parcel) in enumerate(zip(sizes, parcels)):

        @pl.when(origin == k + 1)
        def _(parcel=parcel, size=size):
            put(parcel.at[size * parts], 0)

    @pl.when(origin == 0)
    def _():
        put(last_plane(patches_ref, slot), 0)

    put(after_ref if last is None else parcels[last].at[sizes[last] * parts + 1], 1)

    @pl.loop(0, capacity)
    def _(j):
        for k, parcel in enumerate(parcels):

            @pl.when(plan_ref[0, j] == k + 1)
            def _(parcel=parcel):
                pltpu.make_async_copy(parcel.at[pl.ds(plan_ref[1, j] * parts, parts)], work_ref.at[j], sems.at[j]).start()

    for side in (0, 1):
        pltpu.make_async_copy(patches_ref.at[0, 0], ends_ref.at[side], sems.at[capacity + side]).wait()

    @pl.loop(0, capacity)
    def _(j):
        @pl.when(plan_ref[0, j] > 0)
        def _():
            pltpu.make_async_copy(patches_ref.at[0], work_ref.at[j], sems.at[j]).wait()


def assemble(plan, patches, after, arrived, sizes, last):
    return pl.pallas_call(
        functools.partial(assemble_kernel, sizes, last),
        out_shape=[
            jax.ShapeDtypeStruct(patches.shape, patches.dtype),
            jax.ShapeDtypeStruct((2,) + patches.shape[2:], patches.dtype),
        ],
        grid_spec=pltpu.PrefetchScalarGridSpec(
            num_scalar_prefetch=1,
            grid=(),
            in_specs=[pl.BlockSpec(memory_space=pl.ANY) for _ in range(2 + len(arrived))],
            out_specs=[pl.BlockSpec(memory_space=pl.ANY)] * 2,
            scratch_shapes=[pltpu.SemaphoreType.DMA((patches.shape[0] + 2,))],
        ),
        compiler_params=pltpu.CompilerParams(vmem_limit_bytes=1 << 20),
        name="assemble",
    )(plan, patches, after, *arrived)


def exchange(sizes, last, plan, patches, after):
    parcels = pack(plan, patches, after, sizes, last)
    arrived = [forward(parcel, "blk", 1 + k) for k, parcel in enumerate(parcels)]
    return settle(plan, patches), *assemble(plan, patches, after, arrived, sizes, last)


def body(patches, counts, moves, tags):
    capacity, edge, _ = patches.shape
    steps, devices, groups = (moves.shape[1], lax.axis_size("blk"), lax.axis_size("grp"))
    parcels = min(steps + 1, devices - 1)
    choices = capacity_choices(min(steps, devices - 1), capacity)
    parts = tiled(patches)
    mine = lax.axis_index("blk").astype(jnp.int32).reshape(1, 1)
    row = jnp.pad(jnp.concatenate([counts[:, None], moves, mine], 1), ((0, 0), (0, LANES - steps - 2)))
    given = all_of(lax.optimization_barrier(row), "blk")
    first = parts[0, :SUBLANES, 0]
    line = ("grp", "blk")
    if parcels == devices - 1:
        last = parcels - 1
        after = lax.ppermute(first, line, [((g + 1) * devices, g * devices) for g in range(groups - 1)])
    else:
        last = None
        after = lax.ppermute(first, line, [(i + 1, i) for i in range(groups * devices - 1)])
    plan, picks = make_plan(given, choices, capacity, steps)
    pick = jnp.minimum(picks[0, 0], lax.axis_index("grp") + len(choices))
    branches = [functools.partial(exchange, choice + (0,) * (parcels - len(choice)), last) for choice in choices]
    held, work, ends = lax.switch(pick, branches, plan, parts, after)
    before = lax.ppermute(ends[0], line, [(g * devices, (g + 1) * devices) for g in range(groups - 1)])
    return refine(held, work, plan, tags, ends, before, edge)


def solution(mesh):
    in_specs = (
        P(("grp", "blk"), None, None),
        P(("grp", "blk")),
        P(("grp", "blk"), None),
        P("grp", None),
    )
    out_specs = P(("grp", "blk"), None, None)
    return jax.shard_map(body, mesh=mesh, in_specs=in_specs, out_specs=out_specs, check_vma=False)
```

```python
import functools
import itertools

import jax
import jax.numpy as jnp
import numpy as np
from jax import lax
from jax.experimental import pallas as pl
from jax.experimental.pallas import tpu as pltpu
from jax.sharding import PartitionSpec as P


LANES = 128
SUBLANES = 8
TOGETHER = 2
CHOICES = (
    (4, 3, 3), (5, 4, 4), (3, 2, 2), (2, 4, 2), (2, 2, 2), (3, 5, 3), (3, 3, 3), (5, 2, 2), (4, 2, 2),
    (2, 3, 2), (2, 2, 3), (4, 1, 1), (1, 3, 1), (1, 1, 2), (3, 1, 1), (5, 1, 1), (1, 2, 1), (2, 2, 4),
    (6, 1, 1), (2, 1, 1), (2, 5, 2), (1, 1, 3), (1, 4, 1), (3, 4, 1), (3, 3, 1), (5, 3, 3), (1, 1, 1),
    (3, 2, 1), (1, 5, 1), (2, 2, 1), (2, 3, 1), (3, 1, 2), (4, 3, 1), (2, 1, 2), (4, 2, 1), (1, 2, 2),
)


def refine_table(edge, ghosts):
    finer = np.arange(2 * edge)[:, None]
    coarse = np.arange(edge + 2 * ghosts)[None, :]
    home = finer // 2 + ghosts
    side = home + 2 * (finer % 2) - 1
    return 0.75 * (coarse == home) + 0.25 * (coarse == side)


def window_table(edge):
    inner = LANES // edge - 2
    along_y = refine_table(inner, 1)
    along_z = refine_table(edge, 0)
    table = np.kron(along_y, along_z).T
    return jnp.asarray(np.concatenate([table, table], 0), jnp.bfloat16)


def flat(tiles, across):
    tiles = tiles.reshape(-1, across, tiles.shape[-2], LANES)
    return jnp.concatenate([tiles[:, u].reshape(-1, LANES) for u in range(across)], axis=1)


def refined(middle, before, after, factor, edge, table, rows_ref, put):
    coarse, plane = middle.shape
    across = plane // LANES
    place = lax.broadcasted_iota(jnp.int32, middle.shape, 0)
    below = jnp.where(place == 0, before, pltpu.roll(middle, 1, 0))
    above = jnp.where(place == coarse - 1, after, pltpu.roll(middle, coarse - 1, 0))
    home = middle * (0.75 * factor)
    even = home + below * (0.25 * factor)
    odd = home + above * (0.25 * factor)
    for u in range(across):
        cut = slice(u * LANES, (u + 1) * LANES)
        rows_ref[u, pl.ds(0, coarse, 2), :] = even[:, cut]
        rows_ref[u, pl.ds(1, coarse, 2), :] = odd[:, cut]
    rows = jnp.concatenate([rows_ref[u, : 2 * coarse] for u in range(across)], axis=1)
    lane = lax.broadcasted_iota(jnp.int32, rows.shape, 1)
    later = jnp.where(lane < edge, 0.0, pltpu.roll(rows, edge, 1))
    sooner = jnp.where(lane >= plane - edge, 0.0, pltpu.roll(rows, plane - edge, 1))
    width = table.shape[1]
    pairs = []
    for moved in (later, sooner):
        high = moved.astype(jnp.bfloat16)
        pairs.append((high, (moved - high.astype(jnp.float32)).astype(jnp.bfloat16)))
    for window in range(2 * across):
        cut = slice(window // 2 * LANES, (window // 2 + 1) * LANES)
        left = jnp.concatenate([half[:, cut] for half in pairs[window % 2]], axis=1)
        product = jnp.dot(left, table, preferred_element_type=jnp.float32)
        put(slice(window * width, (window + 1) * width), product.astype(jnp.bfloat16))


def tag_factor(plan_ref, tag_ref, slot):
    return 1.0 + 0.5 * tag_ref[0, plan_ref[2, 1] + slot].astype(jnp.float32)


def refine_kernel(plan_ref, tag_ref, held_ref, work_ref, ends_ref, before_ref, table_ref, out_ref, rows_ref):
    capacity, parts = held_ref.shape[:2]
    together, fine, wide = out_ref.shape
    edge, across = (fine // 2, wide // 4 // LANES)
    base = pl.program_id(0) * together
    live = plan_ref[2, 0]

    @pl.when(base >= live)
    def _():
        out_ref[...] = jnp.zeros_like(out_ref)

    @pl.when(base < live)
    def _():
        def part(j, tiles, rows):
            j = jnp.clip(j, 0, capacity - 1)
            return jnp.where(plan_ref[0, j] == 0, held_ref[j, tiles, rows], work_ref[j, tiles, rows])

        table = table_ref[...]
        lower = jnp.where(plan_ref[2, 4] == 0, ends_ref[0], before_ref[...])[:, None, :]
        for t in range(together):
            slot = base + t
            middle = part(slot, slice(None), slice(None))
            before = part(slot - 1, slice(parts - across, None), slice(SUBLANES - 1, None))
            after = part(slot + 1, slice(0, across), slice(0, 1))
            before = jnp.where(slot == 0, lower, before)
            after = jnp.where(slot == live - 1, ends_ref[1][:, None, :], after)
            factor = tag_factor(plan_ref, tag_ref, jnp.minimum(slot, live - 1))
            if t:
                middle, before, after = (jnp.where(slot < live, x, 0.0) for x in (middle, before, after))

            def put(lanes, values, t=t):
                out_ref[t, :, lanes] = values

            refined(flat(middle, across), flat(before, across), flat(after, across), factor, edge, table, rows_ref.at[t], put)


def refine(held, work, plan, tags, ends, before, edge):
    capacity, parts = work.shape[:2]
    plane = parts * SUBLANES * LANES // edge
    table = window_table(edge)
    together = TOGETHER if capacity % TOGETHER == 0 else 1
    whole = lambda x: pl.BlockSpec(x.shape, lambda i, *_: (0,) * x.ndim)
    operands = (held, work, ends, before, table)
    return pl.pallas_call(
        refine_kernel,
        out_shape=jax.ShapeDtypeStruct((capacity, 2 * edge, 4 * plane), jnp.bfloat16),
        grid_spec=pltpu.PrefetchScalarGridSpec(
            num_scalar_prefetch=2,
            grid=(capacity // together,),
            in_specs=[whole(x) for x in operands],
            out_specs=pl.BlockSpec((together, 2 * edge, 4 * plane), lambda i, *_: (i, 0, 0)),
            scratch_shapes=[pltpu.VMEM((together, plane // LANES, 2 * edge, LANES), jnp.float32)],
        ),
        compiler_params=pltpu.CompilerParams(vmem_limit_bytes=16 << 20),
        name="refine",
    )(plan, tags, *operands)


def swap(block, axis, bit):
    return lax.ppermute(block, axis, [(i, i ^ bit) for i in range(lax.axis_size(axis))])


def all_of(rows, axis):
    count, bit = (lax.axis_size(axis), 1)
    while bit < count:
        other = swap(rows, axis, bit)
        rows = jnp.concatenate([rows, other], 0)
        bit *= 2
    return rows


def forward(block, axis, distance):
    count = lax.axis_size(axis)
    return lax.ppermute(block, axis, [(i, (i + distance) % count) for i in range(count)])


def capacity_choices(distances, capacity):
    most = capacity - 1
    if distances == 3:
        choices = set(CHOICES)
    else:
        choices = {(u,) * distances for u in (1, 2, 3, 4)}
    choices = {tuple(min(c, most) for c in choice) for choice in choices} | {(most,) * distances}
    load = lambda c: (max(a + b for a, b in itertools.combinations(c + (0, 0), 2)), sum(c), c)
    return sorted(choices, key=load)


def tiled(patches):
    capacity, edge, plane = patches.shape
    cut = patches.reshape(capacity, edge // SUBLANES, SUBLANES, plane // LANES, LANES)
    return cut.transpose(0, 1, 3, 2, 4).reshape(capacity, -1, SUBLANES, LANES)


def last_plane(patches_ref, slot):
    return patches_ref.at[slot, pl.ds(patches_ref.shape[1] - SUBLANES, SUBLANES), SUBLANES - 1]


def first_plane(patches_ref, slot):
    return patches_ref.at[slot, pl.ds(0, SUBLANES), 0]


def plan_kernel(given_ref, plan_ref, pick_ref, *, choices, capacity, steps):
    devices = given_ref.shape[0]
    count = devices * max(1, SUBLANES // devices)
    shape = (count, LANES)
    wide = lambda column: jnp.broadcast_to(column, shape)
    behind = lambda x, k: pltpu.roll(x, k % count, 0) if k % count else x
    lane = lax.broadcasted_iota(jnp.int32, shape, 1)
    row = lax.broadcasted_iota(jnp.int32, shape, 0)
    given = given_ref[...]
    mine = given[0:1, steps + 1 : steps + 2]
    rows = jnp.zeros(shape, jnp.int32)
    for f in range(devices):
        ahead = given[f : f + 1, steps + 1 : steps + 2] - mine
        here = row % devices == jnp.where(ahead < 0, ahead + devices, ahead)
        rows = jnp.where(here, wide(given[f : f + 1]), rows)

    def trace(rows):
        starts, live = [], wide(rows[:, 0:1])
        for step in range(steps):
            sent = wide(rows[:, step + 1 : step + 2])
            starts.append(live - sent)
            live = starts[-1] + behind(sent, 1)
        back, place = jnp.zeros(shape, jnp.int32), lane
        for step in reversed(range(steps)):
            here, there = starts[step], behind(starts[step], 1)
            for k in range(1, steps - step):
                here = jnp.where(back == k, behind(starts[step], k), here)
                there = jnp.where(back == k, behind(starts[step], k + 1), there)
            came = place >= here
            place = jnp.where(came, place - here + there, place)
            back = jnp.where(came, back + 1, back)
        for _ in range(steps // devices):
            back = jnp.where(back >= devices, back - devices, back)
        return live, back, place

    def at_top(live, values):
        picked = jnp.where(lane == live - 1, values, 0).astype(jnp.float32)
        return wide(jnp.sum(picked, axis=1, keepdims=True)).astype(jnp.int32)

    live, back, place = trace(rows)
    start_flag = (wide(mine) == 0).astype(jnp.int32)
    top_back = behind(at_top(live, back), 1)
    top_place = jnp.clip(behind(at_top(live, place), 1), 0, capacity - 1)
    top_from = jnp.where(top_back + 1 >= devices, 0, top_back + 1)

    filled = lane < live
    source = jnp.where(filled, back, -1)
    rank = jnp.zeros(shape, jnp.int32)
    for j in range(capacity):
        rank = jnp.where((wide(source[:, j : j + 1]) == source) & (lane > j), rank + 1, rank)
    code = jnp.where(source == row, rank, -1)
    sent = jnp.zeros(shape, jnp.int32)
    for j in range(capacity):
        sent = jnp.where(wide(code[:, j : j + 1]) == lane, wide(place[:, j : j + 1]), sent)
    fits = None
    for k in range(len(choices[0])):
        limit = jnp.full((1, LANES), -1.0, jnp.float32)
        for i, choice in enumerate(choices):
            limit = jnp.where(lane[:1] == i, float(choice[k]), limit)
        hits = jnp.sum((source == k + 1).astype(jnp.float32), axis=1, keepdims=True)
        fit = jnp.max(hits, axis=0, keepdims=True) <= limit
        fits = fit if fits is None else fits & fit
    pick = jnp.min(jnp.where(fits, lane[:1].astype(jnp.float32), LANES - 1.0), axis=1, keepdims=True).astype(jnp.int32)
    pick_ref[...] = jnp.broadcast_to(pick, pick_ref.shape)
    lower = (wide(rows[:, steps + 1 : steps + 2]) < wide(mine)) & (row < devices)
    offset = jnp.sum(jnp.where(lower, live, 0).astype(jnp.float32), axis=0, keepdims=True).astype(jnp.int32)
    kind = jnp.maximum(source, 0)
    index = jnp.where(kind > 0, rank, jnp.where(filled, place, 0))
    values = [wide(live[:1]), wide(offset), wide(top_from[:1]), wide(top_place[:1]), start_flag]
    sizes = values[0]
    for i, value in enumerate(values[1:], 1):
        sizes = jnp.where(lane == i, value, sizes)
    sent = jnp.where(lane == capacity, top_place, sent)
    table = jnp.where(row == 0, wide(kind[:1]), jnp.where(row == 1, wide(index[:1]), sizes))
    plan_ref[...] = jnp.where(row > 2, behind(sent, 2), table)


def make_plan(given, choices, capacity, steps):
    devices = given.shape[0]
    count = devices * max(1, SUBLANES // devices)
    return pl.pallas_call(
        functools.partial(plan_kernel, choices=choices, capacity=capacity, steps=steps),
        out_shape=[jax.ShapeDtypeStruct((rows, LANES), jnp.int32) for rows in (count, 1)],
        in_specs=[pl.BlockSpec(memory_space=pltpu.VMEM)],
        out_specs=[pl.BlockSpec(memory_space=pltpu.VMEM)] * 2,
        compiler_params=pltpu.CompilerParams(vmem_limit_bytes=1 << 20),
        name="plan",
    )(given)


def pack_kernel(sizes, last, plan_ref, patches_ref, after_ref, *refs):
    parcels, sems = refs[:-1], refs[-1]
    capacity, parts = patches_ref.shape[:2]

    def each(act):
        used = 0
        for k, (size, parcel) in enumerate(zip(sizes, parcels)):

            @pl.loop(0, size)
            def _(r, k=k, parcel=parcel, used=used):
                act(pltpu.make_async_copy(patches_ref.at[plan_ref[3 + k, r]], parcel.at[pl.ds(r * parts, parts)], sems.at[used + r]))

            used += size
            act(pltpu.make_async_copy(last_plane(patches_ref, plan_ref[3 + k, capacity]), parcel.at[size * parts], sems.at[used]))
            used += 1
            if k == last:
                upper = parcel.at[size * parts + 1]

                @pl.when(plan_ref[2, 4] == 0)
                def _():
                    act(pltpu.make_async_copy(first_plane(patches_ref, 0), upper, sems.at[used]))

                @pl.when(plan_ref[2, 4] != 0)
                def _():
                    act(pltpu.make_async_copy(after_ref, upper, sems.at[used]))

                used += 1

    each(lambda copy: copy.start())
    each(lambda copy: copy.wait())


def pack(plan, patches, after, sizes, last):
    parts = patches.shape[1]
    return pl.pallas_call(
        functools.partial(pack_kernel, sizes, last),
        out_shape=[
            jax.ShapeDtypeStruct((size * parts + 1 + (k == last),) + patches.shape[2:], patches.dtype)
            for k, size in enumerate(sizes)
        ],
        grid_spec=pltpu.PrefetchScalarGridSpec(
            num_scalar_prefetch=1,
            grid=(),
            in_specs=[pl.BlockSpec(memory_space=pl.ANY)] * 2,
            out_specs=[pl.BlockSpec(memory_space=pl.ANY) for _ in sizes],
            scratch_shapes=[pltpu.SemaphoreType.DMA((sum(sizes) + len(sizes) + 1,))],
        ),
        compiler_params=pltpu.CompilerParams(vmem_limit_bytes=1 << 20),
        name="pack",
    )(plan, patches, after)


def settle_kernel(plan_ref, patches_ref, held_ref, sems):
    def each(act):
        @pl.loop(0, held_ref.shape[0])
        def _(j):
            act(pltpu.make_async_copy(patches_ref.at[plan_ref[1, j]], held_ref.at[j], sems.at[j]))

    each(lambda copy: copy.start())
    each(lambda copy: copy.wait())


def settle(plan, patches):
    return pl.pallas_call(
        settle_kernel,
        out_shape=jax.ShapeDtypeStruct(patches.shape, patches.dtype),
        grid_spec=pltpu.PrefetchScalarGridSpec(
            num_scalar_prefetch=1,
            grid=(),
            in_specs=[pl.BlockSpec(memory_space=pl.ANY)],
            out_specs=pl.BlockSpec(memory_space=pl.ANY),
            scratch_shapes=[pltpu.SemaphoreType.DMA((patches.shape[0],))],
        ),
        compiler_params=pltpu.CompilerParams(vmem_limit_bytes=1 << 20),
        cost_estimate=pl.CostEstimate(flops=1 << 24, bytes_accessed=1 << 21, transcendentals=0),
        name="settle",
    )(plan, patches)


def assemble_kernel(sizes, last, plan_ref, patches_ref, after_ref, *refs):
    parcels, work_ref, ends_ref, sems = refs[:-3], refs[-3], refs[-2], refs[-1]
    capacity, parts = work_ref.shape[:2]

    def put(source, side):
        pltpu.make_async_copy(source, ends_ref.at[side], sems.at[capacity + side]).start()

    origin, slot = plan_ref[2, 2], plan_ref[2, 3]
    for k, (size, parcel) in enumerate(zip(sizes, parcels)):

        @pl.when(origin == k + 1)
        def _(parcel=parcel, size=size):
            put(parcel.at[size * parts], 0)

    @pl.when(origin == 0)
    def _():
        put(last_plane(patches_ref, slot), 0)

    put(after_ref if last is None else parcels[last].at[sizes[last] * parts + 1], 1)

    @pl.loop(0, capacity)
    def _(j):
        for k, parcel in enumerate(parcels):

            @pl.when(plan_ref[0, j] == k + 1)
            def _(parcel=parcel):
                pltpu.make_async_copy(parcel.at[pl.ds(plan_ref[1, j] * parts, parts)], work_ref.at[j], sems.at[j]).start()

    for side in (0, 1):
        pltpu.make_async_copy(patches_ref.at[0, 0], ends_ref.at[side], sems.at[capacity + side]).wait()

    @pl.loop(0, capacity)
    def _(j):
        @pl.when(plan_ref[0, j] > 0)
        def _():
            pltpu.make_async_copy(patches_ref.at[0], work_ref.at[j], sems.at[j]).wait()


def assemble(plan, patches, after, arrived, sizes, last):
    return pl.pallas_call(
        functools.partial(assemble_kernel, sizes, last),
        out_shape=[
            jax.ShapeDtypeStruct(patches.shape, patches.dtype),
            jax.ShapeDtypeStruct((2,) + patches.shape[2:], patches.dtype),
        ],
        grid_spec=pltpu.PrefetchScalarGridSpec(
            num_scalar_prefetch=1,
            grid=(),
            in_specs=[pl.BlockSpec(memory_space=pl.ANY) for _ in range(2 + len(arrived))],
            out_specs=[pl.BlockSpec(memory_space=pl.ANY)] * 2,
            scratch_shapes=[pltpu.SemaphoreType.DMA((patches.shape[0] + 2,))],
        ),
        compiler_params=pltpu.CompilerParams(vmem_limit_bytes=1 << 20),
        name="assemble",
    )(plan, patches, after, *arrived)


def exchange(sizes, last, plan, patches, after):
    parcels = pack(plan, patches, after, sizes, last)
    arrived = [forward(parcel, "blk", 1 + k) for k, parcel in enumerate(parcels)]
    return settle(plan, patches), *assemble(plan, patches, after, arrived, sizes, last)


def body(patches, counts, moves, tags):
    capacity, edge, _ = patches.shape
    steps, devices, groups = (moves.shape[1], lax.axis_size("blk"), lax.axis_size("grp"))
    parcels = min(steps + 1, devices - 1)
    choices = capacity_choices(min(steps, devices - 1), capacity)
    parts = tiled(patches)
    mine = lax.axis_index("blk").astype(jnp.int32).reshape(1, 1)
    row = jnp.pad(jnp.concatenate([counts[:, None], moves, mine], 1), ((0, 0), (0, LANES - steps - 2)))
    given = all_of(lax.optimization_barrier(row), "blk")
    first = parts[0, :SUBLANES, 0]
    line = ("grp", "blk")
    if parcels == devices - 1:
        last = parcels - 1
        after = lax.ppermute(first, line, [((g + 1) * devices, g * devices) for g in range(groups - 1)])
    else:
        last = None
        after = lax.ppermute(first, line, [(i + 1, i) for i in range(groups * devices - 1)])
    plan, picks = make_plan(given, choices, capacity, steps)
    pick = jnp.minimum(picks[0, 0], lax.axis_index("grp") + len(choices))
    branches = [functools.partial(exchange, choice + (0,) * (parcels - len(choice)), last) for choice in choices]
    held, work, ends = lax.switch(pick, branches, plan, parts, after)
    before = lax.ppermute(ends[0], line, [(g * devices, (g + 1) * devices) for g in range(groups - 1)])
    return refine(held, work, plan, tags, ends, before, edge)


def solution(mesh):
    in_specs = (
        P(("grp", "blk"), None, None),
        P(("grp", "blk")),
        P(("grp", "blk"), None),
        P("grp", None),
    )
    out_specs = P(("grp", "blk"), None, None)
    return jax.shard_map(body, mesh=mesh, in_specs=in_specs, out_specs=out_specs, check_vma=False)
```

```python
import functools
import itertools

import jax
import jax.numpy as jnp
import numpy as np
from jax import lax
from jax.experimental import pallas as pl
from jax.experimental.pallas import tpu as pltpu
from jax.sharding import PartitionSpec as P


LANES = 128
SUBLANES = 8
TOGETHER = 2
CHOICES = (
    (4, 3, 3), (5, 4, 4), (3, 2, 2), (2, 4, 2), (2, 2, 2), (3, 5, 3), (3, 3, 3), (5, 2, 2), (4, 2, 2),
    (2, 3, 2), (2, 2, 3), (4, 1, 1), (1, 3, 1), (1, 1, 2), (3, 1, 1), (5, 1, 1), (1, 2, 1), (2, 2, 4),
    (6, 1, 1), (2, 1, 1), (2, 5, 2), (1, 1, 3), (1, 4, 1), (3, 4, 1), (3, 3, 1), (5, 3, 3), (1, 1, 1),
    (3, 2, 1), (1, 5, 1), (2, 2, 1), (2, 3, 1), (3, 1, 2), (4, 3, 1), (2, 1, 2), (4, 2, 1), (1, 2, 2),
)


def refine_table(edge, ghosts):
    finer = np.arange(2 * edge)[:, None]
    coarse = np.arange(edge + 2 * ghosts)[None, :]
    home = finer // 2 + ghosts
    side = home + 2 * (finer % 2) - 1
    return 0.75 * (coarse == home) + 0.25 * (coarse == side)


def window_table(edge):
    inner = LANES // edge - 2
    along_y = refine_table(inner, 1)
    along_z = refine_table(edge, 0)
    table = np.kron(along_y, along_z).T
    return jnp.asarray(np.concatenate([table, table], 0), jnp.bfloat16)


def flat(tiles, across):
    tiles = tiles.reshape(-1, across, tiles.shape[-2], LANES)
    return jnp.concatenate([tiles[:, u].reshape(-1, LANES) for u in range(across)], axis=1)


def refined(middle, before, after, factor, edge, table, rows_ref, put):
    coarse, plane = middle.shape
    across = plane // LANES
    place = lax.broadcasted_iota(jnp.int32, middle.shape, 0)
    below = jnp.where(place == 0, before, pltpu.roll(middle, 1, 0))
    above = jnp.where(place == coarse - 1, after, pltpu.roll(middle, coarse - 1, 0))
    home = middle * (0.75 * factor)
    even = home + below * (0.25 * factor)
    odd = home + above * (0.25 * factor)
    for u in range(across):
        cut = slice(u * LANES, (u + 1) * LANES)
        rows_ref[u, pl.ds(0, coarse, 2), :] = even[:, cut]
        rows_ref[u, pl.ds(1, coarse, 2), :] = odd[:, cut]
    rows = jnp.concatenate([rows_ref[u, : 2 * coarse] for u in range(across)], axis=1)
    lane = lax.broadcasted_iota(jnp.int32, rows.shape, 1)
    later = jnp.where(lane < edge, 0.0, pltpu.roll(rows, edge, 1))
    sooner = jnp.where(lane >= plane - edge, 0.0, pltpu.roll(rows, plane - edge, 1))
    width = table.shape[1]
    pairs = []
    for moved in (later, sooner):
        high = moved.astype(jnp.bfloat16)
        pairs.append((high, (moved - high.astype(jnp.float32)).astype(jnp.bfloat16)))
    for window in range(2 * across):
        cut = slice(window // 2 * LANES, (window // 2 + 1) * LANES)
        left = jnp.concatenate([half[:, cut] for half in pairs[window % 2]], axis=1)
        product = jnp.dot(left, table, preferred_element_type=jnp.float32)
        put(slice(window * width, (window + 1) * width), product.astype(jnp.bfloat16))


def tag_factor(plan_ref, tag_ref, slot):
    return 1.0 + 0.5 * tag_ref[0, plan_ref[2, 1] + slot].astype(jnp.float32)


def refine_kernel(always, plan_ref, tag_ref, held_ref, work_ref, ends_ref, before_ref, after_ref, table_ref, out_ref, rows_ref):
    capacity, parts = held_ref.shape[:2]
    together, fine, wide = out_ref.shape
    edge, across = (fine // 2, wide // 4 // LANES)
    base = pl.program_id(0) * together
    live = plan_ref[2, 0]

    @pl.when(base >= live)
    def _():
        out_ref[...] = jnp.zeros_like(out_ref)

    @pl.when(base < live)
    def _():
        def part(j, tiles, rows):
            j = jnp.clip(j, 0, capacity - 1)
            return jnp.where(plan_ref[0, j] == 0, held_ref[j, tiles, rows], work_ref[j, tiles, rows])

        table = table_ref[...]
        lower = jnp.where(plan_ref[2, 4] == 0, ends_ref[0], before_ref[...])[:, None, :]
        upper = after_ref[...] if always else jnp.where(plan_ref[2, 5] == 0, ends_ref[1], after_ref[...])
        for t in range(together):
            slot = base + t
            middle = part(slot, slice(None), slice(None))
            before = part(slot - 1, slice(parts - across, None), slice(SUBLANES - 1, None))
            after = part(slot + 1, slice(0, across), slice(0, 1))
            before = jnp.where(slot == 0, lower, before)
            after = jnp.where(slot == live - 1, upper[:, None, :], after)
            factor = tag_factor(plan_ref, tag_ref, jnp.minimum(slot, live - 1))
            if t:
                middle, before, after = (jnp.where(slot < live, x, 0.0) for x in (middle, before, after))

            def put(lanes, values, t=t):
                out_ref[t, :, lanes] = values

            refined(flat(middle, across), flat(before, across), flat(after, across), factor, edge, table, rows_ref.at[t], put)


def refine(held, work, plan, tags, ends, before, after, always, edge):
    capacity, parts = work.shape[:2]
    plane = parts * SUBLANES * LANES // edge
    table = window_table(edge)
    together = TOGETHER if capacity % TOGETHER == 0 else 1
    whole = lambda x: pl.BlockSpec(x.shape, lambda i, *_: (0,) * x.ndim)
    operands = (held, work, ends, before, after, table)
    return pl.pallas_call(
        functools.partial(refine_kernel, always),
        out_shape=jax.ShapeDtypeStruct((capacity, 2 * edge, 4 * plane), jnp.bfloat16),
        grid_spec=pltpu.PrefetchScalarGridSpec(
            num_scalar_prefetch=2,
            grid=(capacity // together,),
            in_specs=[whole(x) for x in operands],
            out_specs=pl.BlockSpec((together, 2 * edge, 4 * plane), lambda i, *_: (i, 0, 0)),
            scratch_shapes=[pltpu.VMEM((together, plane // LANES, 2 * edge, LANES), jnp.float32)],
        ),
        compiler_params=pltpu.CompilerParams(vmem_limit_bytes=16 << 20),
        name="refine",
    )(plan, tags, *operands)


def swap(block, axis, bit):
    return lax.ppermute(block, axis, [(i, i ^ bit) for i in range(lax.axis_size(axis))])


def all_of(rows, axis):
    count, bit = (lax.axis_size(axis), 1)
    if count == 4:
        others = []
        for bits in (3, 1, 2):
            others.append(swap(rows, axis, bits))
        return jnp.concatenate([rows, others[1], others[2], others[0]], 0)
    while bit < count:
        other = swap(rows, axis, bit)
        rows = jnp.concatenate([rows, other], 0)
        bit *= 2
    return rows


def forward(block, axis, distance):
    count = lax.axis_size(axis)
    return lax.ppermute(block, axis, [(i, (i + distance) % count) for i in range(count)])


def capacity_choices(distances, capacity):
    most = capacity - 1
    if distances == 3:
        choices = set(CHOICES)
    else:
        choices = {(u,) * distances for u in (1, 2, 3, 4)}
    choices = {tuple(min(c, most) for c in choice) for choice in choices} | {(most,) * distances}
    load = lambda c: (max(a + b for a, b in itertools.combinations(c + (0, 0), 2)), sum(c), c)
    return sorted(choices, key=load)


def tiled(patches):
    capacity, edge, plane = patches.shape
    cut = patches.reshape(capacity, edge // SUBLANES, SUBLANES, plane // LANES, LANES)
    return cut.transpose(0, 1, 3, 2, 4).reshape(capacity, -1, SUBLANES, LANES)


def last_plane(patches_ref, slot):
    return patches_ref.at[slot, pl.ds(patches_ref.shape[1] - SUBLANES, SUBLANES), SUBLANES - 1]


def first_plane(patches_ref, slot):
    return patches_ref.at[slot, pl.ds(0, SUBLANES), 0]


def plan_kernel(given_ref, plan_ref, pick_ref, *, choices, capacity, steps):
    devices = given_ref.shape[0]
    count = devices * max(1, SUBLANES // devices)
    shape = (count, LANES)
    wide = lambda column: jnp.broadcast_to(column, shape)
    behind = lambda x, k: pltpu.roll(x, k % count, 0) if k % count else x
    lane = lax.broadcasted_iota(jnp.int32, shape, 1)
    row = lax.broadcasted_iota(jnp.int32, shape, 0)
    given = given_ref[...]
    mine = given[0:1, steps + 1 : steps + 2]
    rows = jnp.zeros(shape, jnp.int32)
    for f in range(devices):
        ahead = given[f : f + 1, steps + 1 : steps + 2] - mine
        here = row % devices == jnp.where(ahead < 0, ahead + devices, ahead)
        rows = jnp.where(here, wide(given[f : f + 1]), rows)

    def trace(rows):
        starts, live = [], wide(rows[:, 0:1])
        for step in range(steps):
            sent = wide(rows[:, step + 1 : step + 2])
            starts.append(live - sent)
            live = starts[-1] + behind(sent, 1)
        back, place = jnp.zeros(shape, jnp.int32), lane
        for step in reversed(range(steps)):
            here, there = starts[step], behind(starts[step], 1)
            for k in range(1, steps - step):
                here = jnp.where(back == k, behind(starts[step], k), here)
                there = jnp.where(back == k, behind(starts[step], k + 1), there)
            came = place >= here
            place = jnp.where(came, place - here + there, place)
            back = jnp.where(came, back + 1, back)
        for _ in range(steps // devices):
            back = jnp.where(back >= devices, back - devices, back)
        return live, back, place

    def at_top(live, values):
        picked = jnp.where(lane == live - 1, values, 0).astype(jnp.float32)
        return wide(jnp.sum(picked, axis=1, keepdims=True)).astype(jnp.int32)

    live, back, place = trace(rows)
    start_flag = (wide(mine) == 0).astype(jnp.int32)
    top_back = behind(at_top(live, back), 1)
    top_place = jnp.clip(behind(at_top(live, place), 1), 0, capacity - 1)
    top_from = jnp.where(top_back + 1 >= devices, 0, top_back + 1)

    filled = lane < live
    source = jnp.where(filled, back, -1)
    rank = jnp.zeros(shape, jnp.int32)
    for j in range(capacity):
        rank = jnp.where((wide(source[:, j : j + 1]) == source) & (lane > j), rank + 1, rank)
    code = jnp.where(source == row, rank, -1)
    sent = jnp.zeros(shape, jnp.int32)
    for j in range(capacity):
        sent = jnp.where(wide(code[:, j : j + 1]) == lane, wide(place[:, j : j + 1]), sent)
    fits = None
    for k in range(len(choices[0])):
        limit = jnp.full((1, LANES), -1.0, jnp.float32)
        for i, choice in enumerate(choices):
            limit = jnp.where(lane[:1] == i, float(choice[k]), limit)
        hits = jnp.sum((source == k + 1).astype(jnp.float32), axis=1, keepdims=True)
        fit = jnp.max(hits, axis=0, keepdims=True) <= limit
        fits = fit if fits is None else fits & fit
    pick = jnp.min(jnp.where(fits, lane[:1].astype(jnp.float32), LANES - 1.0), axis=1, keepdims=True).astype(jnp.int32)
    pick_ref[...] = jnp.broadcast_to(pick, pick_ref.shape)
    lower = (wide(rows[:, steps + 1 : steps + 2]) < wide(mine)) & (row < devices)
    offset = jnp.sum(jnp.where(lower, live, 0).astype(jnp.float32), axis=0, keepdims=True).astype(jnp.int32)
    kind = jnp.maximum(source, 0)
    index = jnp.where(kind > 0, rank, jnp.where(filled, place, 0))
    values = [wide(live[:1]), wide(offset), wide(top_from[:1]), wide(top_place[:1]), start_flag, (wide(mine) == devices - 1).astype(jnp.int32)]
    sizes = values[0]
    for i, value in enumerate(values[1:], 1):
        sizes = jnp.where(lane == i, value, sizes)
    sent = jnp.where(lane == capacity, top_place, sent)
    table = jnp.where(row == 0, wide(kind[:1]), jnp.where(row == 1, wide(index[:1]), sizes))
    plan_ref[...] = jnp.where(row > 2, behind(sent, 2), table)[:, : plan_ref.shape[1]]


def make_plan(given, choices, capacity, steps):
    devices = given.shape[0]
    count = devices * max(1, SUBLANES // devices)
    return pl.pallas_call(
        functools.partial(plan_kernel, choices=choices, capacity=capacity, steps=steps),
        out_shape=[jax.ShapeDtypeStruct(shape, jnp.int32) for shape in ((count, 2 * SUBLANES), (1, LANES))],
        in_specs=[pl.BlockSpec(memory_space=pltpu.VMEM)],
        out_specs=[pl.BlockSpec(memory_space=pltpu.VMEM)] * 2,
        compiler_params=pltpu.CompilerParams(vmem_limit_bytes=1 << 20),
        name="plan",
    )(given)


def pack_kernel(sizes, last, plan_ref, patches_ref, *refs):
    parcels, sems = refs[:-1], refs[-1]
    capacity, parts = patches_ref.shape[:2]

    def each(act):
        used = 0
        for k, (size, parcel) in enumerate(zip(sizes, parcels)):

            @pl.loop(0, size)
            def _(r, k=k, parcel=parcel, used=used):
                act(pltpu.make_async_copy(patches_ref.at[plan_ref[3 + k, r]], parcel.at[pl.ds(r * parts, parts)], sems.at[used + r]))

            used += size
            act(pltpu.make_async_copy(last_plane(patches_ref, plan_ref[3 + k, capacity]), parcel.at[size * parts], sems.at[used]))
            used += 1
            if k == last:
                act(pltpu.make_async_copy(first_plane(patches_ref, 0), parcel.at[size * parts + 1], sems.at[used]))
                used += 1

    each(lambda copy: copy.start())
    each(lambda copy: copy.wait())


def pack(plan, patches, sizes, last):
    parts = patches.shape[1]
    return pl.pallas_call(
        functools.partial(pack_kernel, sizes, last),
        out_shape=[
            jax.ShapeDtypeStruct((size * parts + 1 + (k == last),) + patches.shape[2:], patches.dtype)
            for k, size in enumerate(sizes)
        ],
        grid_spec=pltpu.PrefetchScalarGridSpec(
            num_scalar_prefetch=1,
            grid=(),
            in_specs=[pl.BlockSpec(memory_space=pl.ANY)],
            out_specs=[pl.BlockSpec(memory_space=pl.ANY) for _ in sizes],
            scratch_shapes=[pltpu.SemaphoreType.DMA((sum(sizes) + len(sizes) + 1,))],
        ),
        compiler_params=pltpu.CompilerParams(vmem_limit_bytes=1 << 20),
        name="pack",
    )(plan, patches)


def settle_kernel(plan_ref, patches_ref, held_ref, sems):
    def each(act):
        @pl.loop(0, held_ref.shape[0])
        def _(j):
            act(pltpu.make_async_copy(patches_ref.at[plan_ref[1, j]], held_ref.at[j], sems.at[j]))

    each(lambda copy: copy.start())
    each(lambda copy: copy.wait())


def settle(plan, patches):
    return pl.pallas_call(
        settle_kernel,
        out_shape=jax.ShapeDtypeStruct(patches.shape, patches.dtype),
        grid_spec=pltpu.PrefetchScalarGridSpec(
            num_scalar_prefetch=1,
            grid=(),
            in_specs=[pl.BlockSpec(memory_space=pl.ANY)],
            out_specs=pl.BlockSpec(memory_space=pl.ANY),
            scratch_shapes=[pltpu.SemaphoreType.DMA((patches.shape[0],))],
        ),
        compiler_params=pltpu.CompilerParams(vmem_limit_bytes=1 << 20),
        cost_estimate=pl.CostEstimate(flops=1 << 24, bytes_accessed=1 << 21, transcendentals=0),
        name="settle",
    )(plan, patches)


def assemble_kernel(sizes, last, plan_ref, patches_ref, *refs):
    parcels, work_ref, ends_ref, sems = refs[:-3], refs[-3], refs[-2], refs[-1]
    capacity, parts = work_ref.shape[:2]

    def put(source, side):
        pltpu.make_async_copy(source, ends_ref.at[side], sems.at[capacity + side]).start()

    origin, slot = plan_ref[2, 2], plan_ref[2, 3]
    for k, (size, parcel) in enumerate(zip(sizes, parcels)):

        @pl.when(origin == k + 1)
        def _(parcel=parcel, size=size):
            put(parcel.at[size * parts], 0)

    @pl.when(origin == 0)
    def _():
        put(last_plane(patches_ref, slot), 0)

    put(first_plane(patches_ref, 0) if last is None else parcels[last].at[sizes[last] * parts + 1], 1)
    put(first_plane(patches_ref, 0), 2)

    @pl.loop(0, capacity)
    def _(j):
        for k, parcel in enumerate(parcels):

            @pl.when(plan_ref[0, j] == k + 1)
            def _(parcel=parcel):
                pltpu.make_async_copy(parcel.at[pl.ds(plan_ref[1, j] * parts, parts)], work_ref.at[j], sems.at[j]).start()

    for side in range(3):
        pltpu.make_async_copy(patches_ref.at[0, 0], ends_ref.at[side], sems.at[capacity + side]).wait()

    @pl.loop(0, capacity)
    def _(j):
        @pl.when(plan_ref[0, j] > 0)
        def _():
            pltpu.make_async_copy(patches_ref.at[0], work_ref.at[j], sems.at[j]).wait()


def assemble(plan, patches, arrived, sizes, last):
    return pl.pallas_call(
        functools.partial(assemble_kernel, sizes, last),
        out_shape=[
            jax.ShapeDtypeStruct(patches.shape, patches.dtype),
            jax.ShapeDtypeStruct((3,) + patches.shape[2:], patches.dtype),
        ],
        grid_spec=pltpu.PrefetchScalarGridSpec(
            num_scalar_prefetch=1,
            grid=(),
            in_specs=[pl.BlockSpec(memory_space=pl.ANY) for _ in range(1 + len(arrived))],
            out_specs=[pl.BlockSpec(memory_space=pl.ANY)] * 2,
            scratch_shapes=[pltpu.SemaphoreType.DMA((patches.shape[0] + 3,))],
        ),
        compiler_params=pltpu.CompilerParams(vmem_limit_bytes=1 << 20),
        name="assemble",
    )(plan, patches, *arrived)


def exchange(sizes, last, plan, patches):
    parcels = pack(plan, patches, sizes, last)
    arrived = [forward(parcel, "blk", 1 + k) for k, parcel in enumerate(parcels)]
    return settle(plan, patches), *assemble(plan, patches, arrived, sizes, last)


def body(patches, counts, moves, tags):
    capacity, edge, _ = patches.shape
    steps, devices, groups = (moves.shape[1], lax.axis_size("blk"), lax.axis_size("grp"))
    parcels = min(steps + 1, devices - 1)
    choices = capacity_choices(min(steps, devices - 1), capacity)
    parts = tiled(patches)
    mine = lax.axis_index("blk").astype(jnp.int32).reshape(1, 1)
    row = jnp.pad(jnp.concatenate([counts[:, None], moves, mine], 1), ((0, 0), (0, LANES - steps - 2)))
    given = all_of(lax.optimization_barrier(row), "blk")
    line = ("grp", "blk")
    last = parcels - 1 if parcels == devices - 1 else None
    plan, picks = make_plan(given, choices, capacity, steps)
    pick = jnp.minimum(picks[0, 0], lax.axis_index("grp") + len(choices))
    branches = [functools.partial(exchange, choice + (0,) * (parcels - len(choice)), last) for choice in choices]
    held, work, ends = lax.switch(pick, branches, plan, parts)
    before = lax.ppermute(ends[0], line, [(g * devices, (g + 1) * devices) for g in range(groups - 1)])
    stride = 1 if last is None else devices
    after = lax.ppermute(ends[2], line, [(i, i - 1) for i in range(stride, groups * devices, stride)])
    return refine(held, work, plan, tags, ends, before, after, last is None, edge)


def solution(mesh):
    in_specs = (
        P(("grp", "blk"), None, None),
        P(("grp", "blk")),
        P(("grp", "blk"), None),
        P("grp", None),
    )
    out_specs = P(("grp", "blk"), None, None)
    return jax.shard_map(body, mesh=mesh, in_specs=in_specs, out_specs=out_specs, check_vma=False)
```

```python
import functools
import itertools

import jax
import jax.numpy as jnp
import numpy as np
from jax import lax
from jax.experimental import pallas as pl
from jax.experimental.pallas import tpu as pltpu
from jax.sharding import PartitionSpec as P


LANES = 128
SUBLANES = 8
TOGETHER = 2
CHOICES = (
    (0, 2, 3), (1, 1, 1), (1, 1, 2), (1, 1, 3), (1, 2, 1), (1, 2, 2), (1, 3, 1), (1, 3, 2), (1, 3, 3),
    (1, 4, 1), (1, 5, 1), (2, 1, 1), (2, 1, 2), (2, 1, 3), (2, 2, 1), (2, 2, 2), (2, 2, 3), (2, 2, 4),
    (2, 3, 1), (2, 3, 2), (2, 4, 1), (2, 4, 2), (2, 5, 2), (3, 1, 1), (3, 1, 2), (3, 1, 3), (3, 2, 1),
    (3, 2, 2), (3, 3, 0), (3, 3, 1), (3, 3, 3), (3, 4, 1), (3, 5, 3), (4, 1, 1), (4, 1, 2), (4, 1, 3),
    (4, 2, 1), (4, 2, 2), (4, 3, 1), (4, 3, 3), (5, 1, 1), (5, 1, 2), (5, 2, 1), (5, 2, 2), (5, 3, 0),
    (5, 3, 3), (5, 4, 4), (6, 1, 1), (6, 5, 4),
)


def refine_table(edge, ghosts):
    finer = np.arange(2 * edge)[:, None]
    coarse = np.arange(edge + 2 * ghosts)[None, :]
    home = finer // 2 + ghosts
    side = home + 2 * (finer % 2) - 1
    return 0.75 * (coarse == home) + 0.25 * (coarse == side)


def window_table(edge):
    inner = LANES // edge - 2
    along_y = refine_table(inner, 1)
    along_z = refine_table(edge, 0)
    table = np.kron(along_y, along_z).T
    return jnp.asarray(np.concatenate([table, table], 0), jnp.bfloat16)


def flat(tiles, across):
    tiles = tiles.reshape(-1, across, tiles.shape[-2], LANES)
    return jnp.concatenate([tiles[:, u].reshape(-1, LANES) for u in range(across)], axis=1)


def refined(middle, before, after, factor, edge, table, rows_ref, put):
    coarse, plane = middle.shape
    across = plane // LANES
    place = lax.broadcasted_iota(jnp.int32, middle.shape, 0)
    below = jnp.where(place == 0, before, pltpu.roll(middle, 1, 0))
    above = jnp.where(place == coarse - 1, after, pltpu.roll(middle, coarse - 1, 0))
    home = middle * (0.75 * factor)
    even = home + below * (0.25 * factor)
    odd = home + above * (0.25 * factor)
    for u in range(across):
        cut = slice(u * LANES, (u + 1) * LANES)
        rows_ref[u, pl.ds(0, coarse, 2), :] = even[:, cut]
        rows_ref[u, pl.ds(1, coarse, 2), :] = odd[:, cut]
    rows = jnp.concatenate([rows_ref[u, : 2 * coarse] for u in range(across)], axis=1)
    lane = lax.broadcasted_iota(jnp.int32, rows.shape, 1)
    later = jnp.where(lane < edge, 0.0, pltpu.roll(rows, edge, 1))
    sooner = jnp.where(lane >= plane - edge, 0.0, pltpu.roll(rows, plane - edge, 1))
    width = table.shape[1]
    pairs = []
    for moved in (later, sooner):
        high = moved.astype(jnp.bfloat16)
        pairs.append((high, (moved - high.astype(jnp.float32)).astype(jnp.bfloat16)))
    for window in range(2 * across):
        cut = slice(window // 2 * LANES, (window // 2 + 1) * LANES)
        left = jnp.concatenate([half[:, cut] for half in pairs[window % 2]], axis=1)
        product = jnp.dot(left, table, preferred_element_type=jnp.float32)
        put(slice(window * width, (window + 1) * width), product.astype(jnp.bfloat16))


def tag_factor(plan_ref, tag_ref, slot):
    return 1.0 + 0.5 * tag_ref[0, plan_ref[2, 1] + slot].astype(jnp.float32)


def refine_kernel(always, plan_ref, tag_ref, held_ref, work_ref, ends_ref, before_ref, after_ref, table_ref, out_ref, rows_ref):
    capacity, parts = held_ref.shape[:2]
    together, fine, wide = out_ref.shape
    edge, across = (fine // 2, wide // 4 // LANES)
    base = pl.program_id(0) * together
    live = plan_ref[2, 0]

    @pl.when(base >= live)
    def _():
        out_ref[...] = jnp.zeros_like(out_ref)

    @pl.when(base < live)
    def _():
        def part(j, tiles, rows):
            j = jnp.clip(j, 0, capacity - 1)
            return jnp.where(plan_ref[0, j] == 0, held_ref[j, tiles, rows], work_ref[j, tiles, rows])

        table = table_ref[...]
        lower = jnp.where(plan_ref[2, 4] == 0, ends_ref[0], before_ref[...])[:, None, :]
        upper = after_ref[...] if always else jnp.where(plan_ref[2, 5] == 0, ends_ref[1], after_ref[...])
        for t in range(together):
            slot = base + t
            middle = part(slot, slice(None), slice(None))
            before = part(slot - 1, slice(parts - across, None), slice(SUBLANES - 1, None))
            after = part(slot + 1, slice(0, across), slice(0, 1))
            before = jnp.where(slot == 0, lower, before)
            after = jnp.where(slot == live - 1, upper[:, None, :], after)
            factor = tag_factor(plan_ref, tag_ref, jnp.minimum(slot, live - 1))
            if t:
                middle, before, after = (jnp.where(slot < live, x, 0.0) for x in (middle, before, after))

            def put(lanes, values, t=t):
                out_ref[t, :, lanes] = values

            refined(flat(middle, across), flat(before, across), flat(after, across), factor, edge, table, rows_ref.at[t], put)


def refine(held, work, plan, tags, ends, before, after, always, edge):
    capacity, parts = work.shape[:2]
    plane = parts * SUBLANES * LANES // edge
    table = window_table(edge)
    together = TOGETHER if capacity % TOGETHER == 0 else 1
    whole = lambda x: pl.BlockSpec(x.shape, lambda i, *_: (0,) * x.ndim)
    operands = (held, work, ends, before, after, table)
    return pl.pallas_call(
        functools.partial(refine_kernel, always),
        out_shape=jax.ShapeDtypeStruct((capacity, 2 * edge, 4 * plane), jnp.bfloat16),
        grid_spec=pltpu.PrefetchScalarGridSpec(
            num_scalar_prefetch=2,
            grid=(capacity // together,),
            in_specs=[whole(x) for x in operands],
            out_specs=pl.BlockSpec((together, 2 * edge, 4 * plane), lambda i, *_: (i, 0, 0)),
            scratch_shapes=[pltpu.VMEM((together, plane // LANES, 2 * edge, LANES), jnp.float32)],
        ),
        compiler_params=pltpu.CompilerParams(vmem_limit_bytes=16 << 20),
        name="refine",
    )(plan, tags, *operands)


def swap(block, axis, bit):
    return lax.ppermute(block, axis, [(i, i ^ bit) for i in range(lax.axis_size(axis))])


def all_of(rows, axis):
    count, bit = (lax.axis_size(axis), 1)
    if count == 4:
        others = []
        for bits in (3, 1, 2):
            others.append(swap(rows, axis, bits))
        return jnp.concatenate([rows, others[1], others[2], others[0]], 0)
    while bit < count:
        other = swap(rows, axis, bit)
        rows = jnp.concatenate([rows, other], 0)
        bit *= 2
    return rows


def forward(block, axis, distance):
    count = lax.axis_size(axis)
    return lax.ppermute(block, axis, [(i, (i + distance) % count) for i in range(count)])


def capacity_choices(distances, capacity):
    most = capacity - 1
    if distances == 3:
        choices = set(CHOICES)
    else:
        choices = {(u,) * distances for u in (1, 2, 3, 4)}
    choices = {tuple(min(c, most) for c in choice) for choice in choices} | {(most,) * distances}
    load = lambda c: (max(a + b for a, b in itertools.combinations(c + (0, 0), 2)) + 0.05 * sum(c), c)
    return sorted(choices, key=load)


def tiled(patches):
    capacity, edge, plane = patches.shape
    cut = patches.reshape(capacity, edge // SUBLANES, SUBLANES, plane // LANES, LANES)
    return cut.transpose(0, 1, 3, 2, 4).reshape(capacity, -1, SUBLANES, LANES)


def last_plane(patches_ref, slot):
    return patches_ref.at[slot, pl.ds(patches_ref.shape[1] - SUBLANES, SUBLANES), SUBLANES - 1]


def first_plane(patches_ref, slot):
    return patches_ref.at[slot, pl.ds(0, SUBLANES), 0]


def plan_kernel(given_ref, plan_ref, pick_ref, *, choices, capacity, steps):
    devices = given_ref.shape[0]
    count = devices * max(1, SUBLANES // devices)
    shape = (count, LANES)
    wide = lambda column: jnp.broadcast_to(column, shape)
    behind = lambda x, k: pltpu.roll(x, k % count, 0) if k % count else x
    lane = lax.broadcasted_iota(jnp.int32, shape, 1)
    row = lax.broadcasted_iota(jnp.int32, shape, 0)
    given = given_ref[...]
    mine = given[0:1, steps + 1 : steps + 2]
    rows = jnp.zeros(shape, jnp.int32)
    for f in range(devices):
        ahead = given[f : f + 1, steps + 1 : steps + 2] - mine
        here = row % devices == jnp.where(ahead < 0, ahead + devices, ahead)
        rows = jnp.where(here, wide(given[f : f + 1]), rows)

    def trace(rows):
        starts, live = [], wide(rows[:, 0:1])
        for step in range(steps):
            sent = wide(rows[:, step + 1 : step + 2])
            starts.append(live - sent)
            live = starts[-1] + behind(sent, 1)
        back, place = jnp.zeros(shape, jnp.int32), lane
        for step in reversed(range(steps)):
            here, there = starts[step], behind(starts[step], 1)
            for k in range(1, steps - step):
                here = jnp.where(back == k, behind(starts[step], k), here)
                there = jnp.where(back == k, behind(starts[step], k + 1), there)
            came = place >= here
            place = jnp.where(came, place - here + there, place)
            back = jnp.where(came, back + 1, back)
        for _ in range(steps // devices):
            back = jnp.where(back >= devices, back - devices, back)
        return live, back, place

    def at_top(live, values):
        picked = jnp.where(lane == live - 1, values, 0).astype(jnp.float32)
        return wide(jnp.sum(picked, axis=1, keepdims=True)).astype(jnp.int32)

    live, back, place = trace(rows)
    start_flag = (wide(mine) == 0).astype(jnp.int32)
    top_back = behind(at_top(live, back), 1)
    top_place = jnp.clip(behind(at_top(live, place), 1), 0, capacity - 1)
    top_from = jnp.where(top_back + 1 >= devices, 0, top_back + 1)

    filled = lane < live
    source = jnp.where(filled, back, -1)
    rank = jnp.zeros(shape, jnp.int32)
    for j in range(capacity):
        rank = jnp.where((wide(source[:, j : j + 1]) == source) & (lane > j), rank + 1, rank)
    code = jnp.where(source == row, rank, -1)
    sent = jnp.zeros(shape, jnp.int32)
    for j in range(capacity):
        sent = jnp.where(wide(code[:, j : j + 1]) == lane, wide(place[:, j : j + 1]), sent)
    fits = None
    for k in range(len(choices[0])):
        limit = jnp.full((1, LANES), -1.0, jnp.float32)
        for i, choice in enumerate(choices):
            limit = jnp.where(lane[:1] == i, float(choice[k]), limit)
        hits = jnp.sum((source == k + 1).astype(jnp.float32), axis=1, keepdims=True)
        fit = jnp.max(hits, axis=0, keepdims=True) <= limit
        fits = fit if fits is None else fits & fit
    pick = jnp.min(jnp.where(fits, lane[:1].astype(jnp.float32), LANES - 1.0), axis=1, keepdims=True).astype(jnp.int32)
    pick_ref[...] = jnp.broadcast_to(pick, pick_ref.shape)
    lower = (wide(rows[:, steps + 1 : steps + 2]) < wide(mine)) & (row < devices)
    offset = jnp.sum(jnp.where(lower, live, 0).astype(jnp.float32), axis=0, keepdims=True).astype(jnp.int32)
    kind = jnp.maximum(source, 0)
    index = jnp.where(kind > 0, rank, jnp.where(filled, place, 0))
    values = [wide(live[:1]), wide(offset), wide(top_from[:1]), wide(top_place[:1]), start_flag, (wide(mine) == devices - 1).astype(jnp.int32)]
    sizes = values[0]
    for i, value in enumerate(values[1:], 1):
        sizes = jnp.where(lane == i, value, sizes)
    sent = jnp.where(lane == capacity, top_place, sent)
    table = jnp.where(row == 0, wide(kind[:1]), jnp.where(row == 1, wide(index[:1]), sizes))
    plan_ref[...] = jnp.where(row > 2, behind(sent, 2), table)[:, : plan_ref.shape[1]]


def make_plan(given, choices, capacity, steps):
    devices = given.shape[0]
    count = devices * max(1, SUBLANES // devices)
    return pl.pallas_call(
        functools.partial(plan_kernel, choices=choices, capacity=capacity, steps=steps),
        out_shape=[jax.ShapeDtypeStruct(shape, jnp.int32) for shape in ((count, 2 * SUBLANES), (1, LANES))],
        in_specs=[pl.BlockSpec(memory_space=pltpu.VMEM)],
        out_specs=[pl.BlockSpec(memory_space=pltpu.VMEM)] * 2,
        compiler_params=pltpu.CompilerParams(vmem_limit_bytes=1 << 20),
        name="plan",
    )(given)


def pack_kernel(sizes, last, plan_ref, patches_ref, *refs):
    parcels, sems = refs[:-1], refs[-1]
    capacity, parts = patches_ref.shape[:2]

    def each(act):
        used = 0
        for k, (size, parcel) in enumerate(zip(sizes, parcels)):

            @pl.loop(0, size)
            def _(r, k=k, parcel=parcel, used=used):
                act(pltpu.make_async_copy(patches_ref.at[plan_ref[3 + k, r]], parcel.at[pl.ds(r * parts, parts)], sems.at[used + r]))

            used += size
            act(pltpu.make_async_copy(last_plane(patches_ref, plan_ref[3 + k, capacity]), parcel.at[size * parts], sems.at[used]))
            used += 1
            if k == last:
                act(pltpu.make_async_copy(first_plane(patches_ref, 0), parcel.at[size * parts + 1], sems.at[used]))
                used += 1

    each(lambda copy: copy.start())
    each(lambda copy: copy.wait())


def pack(plan, patches, sizes, last):
    parts = patches.shape[1]
    return pl.pallas_call(
        functools.partial(pack_kernel, sizes, last),
        out_shape=[
            jax.ShapeDtypeStruct((size * parts + 1 + (k == last),) + patches.shape[2:], patches.dtype)
            for k, size in enumerate(sizes)
        ],
        grid_spec=pltpu.PrefetchScalarGridSpec(
            num_scalar_prefetch=1,
            grid=(),
            in_specs=[pl.BlockSpec(memory_space=pl.ANY)],
            out_specs=[pl.BlockSpec(memory_space=pl.ANY) for _ in sizes],
            scratch_shapes=[pltpu.SemaphoreType.DMA((sum(sizes) + len(sizes) + 1,))],
        ),
        compiler_params=pltpu.CompilerParams(vmem_limit_bytes=1 << 20),
        name="pack",
    )(plan, patches)


def settle_kernel(plan_ref, patches_ref, held_ref, sems):
    def each(act):
        @pl.loop(0, held_ref.shape[0])
        def _(j):
            act(pltpu.make_async_copy(patches_ref.at[plan_ref[1, j]], held_ref.at[j], sems.at[j]))

    each(lambda copy: copy.start())
    each(lambda copy: copy.wait())


def settle(plan, patches):
    return pl.pallas_call(
        settle_kernel,
        out_shape=jax.ShapeDtypeStruct(patches.shape, patches.dtype),
        grid_spec=pltpu.PrefetchScalarGridSpec(
            num_scalar_prefetch=1,
            grid=(),
            in_specs=[pl.BlockSpec(memory_space=pl.ANY)],
            out_specs=pl.BlockSpec(memory_space=pl.ANY),
            scratch_shapes=[pltpu.SemaphoreType.DMA((patches.shape[0],))],
        ),
        compiler_params=pltpu.CompilerParams(vmem_limit_bytes=1 << 20),
        cost_estimate=pl.CostEstimate(flops=1 << 24, bytes_accessed=1 << 21, transcendentals=0),
        name="settle",
    )(plan, patches)


def assemble_kernel(sizes, last, plan_ref, patches_ref, *refs):
    parcels, work_ref, ends_ref, sems = refs[:-3], refs[-3], refs[-2], refs[-1]
    capacity, parts = work_ref.shape[:2]

    def put(source, side):
        pltpu.make_async_copy(source, ends_ref.at[side], sems.at[capacity + side]).start()

    origin, slot = plan_ref[2, 2], plan_ref[2, 3]
    for k, (size, parcel) in enumerate(zip(sizes, parcels)):

        @pl.when(origin == k + 1)
        def _(parcel=parcel, size=size):
            put(parcel.at[size * parts], 0)

    @pl.when(origin == 0)
    def _():
        put(last_plane(patches_ref, slot), 0)

    put(first_plane(patches_ref, 0) if last is None else parcels[last].at[sizes[last] * parts + 1], 1)
    put(first_plane(patches_ref, 0), 2)

    @pl.loop(0, capacity)
    def _(j):
        for k, parcel in enumerate(parcels):

            @pl.when(plan_ref[0, j] == k + 1)
            def _(parcel=parcel):
                pltpu.make_async_copy(parcel.at[pl.ds(plan_ref[1, j] * parts, parts)], work_ref.at[j], sems.at[j]).start()

    for side in range(3):
        pltpu.make_async_copy(patches_ref.at[0, 0], ends_ref.at[side], sems.at[capacity + side]).wait()

    @pl.loop(0, capacity)
    def _(j):
        @pl.when(plan_ref[0, j] > 0)
        def _():
            pltpu.make_async_copy(patches_ref.at[0], work_ref.at[j], sems.at[j]).wait()


def assemble(plan, patches, arrived, sizes, last):
    return pl.pallas_call(
        functools.partial(assemble_kernel, sizes, last),
        out_shape=[
            jax.ShapeDtypeStruct(patches.shape, patches.dtype),
            jax.ShapeDtypeStruct((3,) + patches.shape[2:], patches.dtype),
        ],
        grid_spec=pltpu.PrefetchScalarGridSpec(
            num_scalar_prefetch=1,
            grid=(),
            in_specs=[pl.BlockSpec(memory_space=pl.ANY) for _ in range(1 + len(arrived))],
            out_specs=[pl.BlockSpec(memory_space=pl.ANY)] * 2,
            scratch_shapes=[pltpu.SemaphoreType.DMA((patches.shape[0] + 3,))],
        ),
        compiler_params=pltpu.CompilerParams(vmem_limit_bytes=1 << 20),
        name="assemble",
    )(plan, patches, *arrived)


def exchange(sizes, last, plan, patches):
    parcels = pack(plan, patches, sizes, last)
    arrived = [forward(parcel, "blk", 1 + k) for k, parcel in enumerate(parcels)]
    return settle(plan, patches), *assemble(plan, patches, arrived, sizes, last)


def body(patches, counts, moves, tags):
    capacity, edge, _ = patches.shape
    steps, devices, groups = (moves.shape[1], lax.axis_size("blk"), lax.axis_size("grp"))
    parcels = min(steps + 1, devices - 1)
    choices = capacity_choices(min(steps, devices - 1), capacity)
    parts = tiled(patches)
    mine = lax.axis_index("blk").astype(jnp.int32).reshape(1, 1)
    row = jnp.pad(jnp.concatenate([counts[:, None], moves, mine], 1), ((0, 0), (0, LANES - steps - 2)))
    given = all_of(lax.optimization_barrier(row), "blk")
    line = ("grp", "blk")
    last = parcels - 1 if parcels == devices - 1 else None
    plan, picks = make_plan(given, choices, capacity, steps)
    pick = jnp.minimum(picks[0, 0], lax.axis_index("grp") + len(choices))
    branches = [functools.partial(exchange, choice + (0,) * (parcels - len(choice)), last) for choice in choices]
    held, work, ends = lax.switch(pick, branches, plan, parts)
    before = lax.ppermute(ends[0], line, [(g * devices, (g + 1) * devices) for g in range(groups - 1)])
    stride = 1 if last is None else devices
    after = lax.ppermute(ends[2], line, [(i, i - 1) for i in range(stride, groups * devices, stride)])
    return refine(held, work, plan, tags, ends, before, after, last is None, edge)


def solution(mesh):
    in_specs = (
        P(("grp", "blk"), None, None),
        P(("grp", "blk")),
        P(("grp", "blk"), None),
        P("grp", None),
    )
    out_specs = P(("grp", "blk"), None, None)
    return jax.shard_map(body, mesh=mesh, in_specs=in_specs, out_specs=out_specs, check_vma=False)
```
